32 devices in a mesh: groups: 2 (over y), fsdp: 4 (over z), tensor: 4 (over x, core).
Axes of the slice: x: 2, y: 2, z: 4, core: 2. Of those that a mesh axis runs over, the one named last changes fastest.
Arguments:
- tokens: bfloat16 [2048, 4608], P(('groups', 'fsdp'), 'tensor'), parts along dimension 0, may hold values from -100 to 100
- norm_gain: bfloat16 [4608], P('tensor'), may hold values from 0.25 to 1.75
- w_query: bfloat16 [4608, 4096], P('fsdp', 'tensor'), may hold values from -0.5 to 0.5
- w_key: bfloat16 [4608, 2048], P('fsdp', 'tensor'), may hold values from -0.09375 to 0.09375
- w_value: bfloat16 [4608, 2048], P('fsdp', 'tensor'), may hold values from -0.09375 to 0.09375
- w_out: bfloat16 [4096, 4608], P('tensor', 'fsdp'), may hold values from -0.5 to 0.5
- post_gain: bfloat16 [4608], P('tensor'), may hold values from 0.25 to 1.75
Outputs:
- mixed: float32 [2048, 4608], P(('groups', 'fsdp'), 'tensor'), parts along dimension 0
The draws below stay inside these ranges and needn't reach their ends.
There are 2 independent parts, one for each index of `groups`. The reference program is written for one: setup_inputs(seed, part) draws one part's arguments, and reference() takes and returns one part's arrays. A program takes and returns all parts, laid end to end along the dimension named above; an argument that names none is the same for every part. Nothing has to cross between parts.
All inputs are finite; a program needn't handle non-finite values.
Results may differ from the reference program's by a relative error of at most 0.0053.
Values may be sent and summed in bfloat16 or wider, within the bound.
A program may use at most 128 MiB of HBM per device.

```python
import jax
import jax.numpy as jnp
from jax import lax

D = 4608
HEAD_DIM = 128
HEADS = 32
KV_HEADS = 16
LEN = 256
TOKENS = 1024
BLOCK_COLS = 1024
N_TENSOR = 4


def draw_tokens(key, part):
    base_key, col_key, row_key = jax.random.split(key, 3)
    col = jnp.arange(D, dtype=jnp.float32) / D
    col_scale = 10.0 ** (col - 0.5 + 0.3 * jax.random.uniform(col_key, (D,), jnp.float32, -1.0, 1.0))
    row_scale = 10.0 ** jax.random.uniform(row_key, (TOKENS, 1), jnp.float32, -0.5, 0.5)
    base = jnp.clip(jax.random.normal(base_key, (TOKENS, D), jnp.float32), -5.0, 5.0)
    return (base * row_scale * col_scale[None, :]).astype(jnp.bfloat16)


def draw_w_out(key, part):
    base_key, col_key = jax.random.split(key, 2)
    rows = HEADS * HEAD_DIM
    col = jnp.arange(D, dtype=jnp.float32) / D
    col_scale = 10.0 ** (0.8 * col - 0.4 + 0.2 * jax.random.uniform(col_key, (D,), jnp.float32, -1.0, 1.0))
    base = jnp.clip(jax.random.normal(base_key, (rows, D), jnp.float32), -5.0, 5.0)
    return (base * col_scale[None, :] / jnp.sqrt(jnp.float32(rows))).astype(jnp.bfloat16)


def shard_levels(stream_key, dims, cuts, least, largest):
    def one(dim, blocks):
        heights = jax.random.uniform(jax.random.fold_in(jax.random.fold_in(stream_key, 6), dim), (blocks,), jnp.float32, least / len(cuts), largest / len(cuts))
        return jnp.repeat(jnp.exp(heights), dims[dim] // blocks).reshape((-1,) + (1,) * (len(dims) - dim - 1))

    factor_of = one(*cuts[0])
    for cut in cuts[1:]:
        factor_of = factor_of * one(*cut)
    return factor_of


def normal_values(rng, extent, spread, limit, shards=(), kind=jnp.bfloat16):
    level = shard_levels(rng, extent, shards, -0.22, 0.18) if shards else 1.0
    array = jax.random.normal(rng, extent, jnp.float32) * spread * level
    return jnp.minimum(jnp.maximum(array, -limit), limit).astype(kind)


def setup_inputs(seed: int = 0, part: int = 0) -> dict:
    streams_of = jax.random.split(jax.random.key(seed), 8)
    part_splits = jax.random.split(jax.random.fold_in(streams_of[7], part), 8)
    tokens = draw_tokens(jax.random.fold_in(jax.random.fold_in(streams_of[7], part), 71), part)
    norm_gain = jnp.clip(1.0 + 0.15 * jax.random.normal(streams_of[1], (D,), jnp.float32), 0.25, 1.75).astype(jnp.bfloat16)
    w_query = normal_values(streams_of[2], (D, HEADS * HEAD_DIM), (D // 36) ** -0.5, 0.5, ((0, 4), (1, 4)))
    w_key = normal_values(streams_of[3], (D, KV_HEADS * HEAD_DIM), D ** -0.5, 0.09375, ((0, 4), (1, 4)))
    w_value = normal_values(streams_of[4], (D, KV_HEADS * HEAD_DIM), D ** -0.5, 0.09375, ((0, 4), (1, 4)))
    w_out = draw_w_out(jax.random.fold_in(streams_of[7], 71), part)
    post_gain = jnp.clip(1.0 + 0.15 * jax.random.normal(streams_of[6], (D,), jnp.float32), 0.25, 1.75).astype(jnp.bfloat16)
    return {"tokens": tokens, "norm_gain": norm_gain, "w_query": w_query, "w_key": w_key, "w_value": w_value, "w_out": w_out, "post_gain": post_gain}


eps_norm = 1e-06
soft_cap = 50.0
attn_scale = 144.0 ** (-0.5)
rope_base = 10000.0

def rotate(values, position):
    head_dim = values.shape[-1]
    half = head_dim // 2
    freq = rope_base ** (-(jnp.arange(half, dtype=jnp.float32) * 2.0 / head_dim))
    angle = position.astype(jnp.float32)[:, None] * freq[None, :]
    cosine = jnp.cos(angle)[:, None, :]
    sine = jnp.sin(angle)[:, None, :]
    first = values[..., :half]
    second = values[..., half:]
    return jnp.concatenate([first * cosine - second * sine, second * cosine + first * sine], axis=-1)

def attend(query, keys, values):
    count, heads, head_dim = query.shape
    kv_count = keys.shape[1]
    grouped = query.reshape(count, kv_count, heads // kv_count, head_dim).astype(jnp.float32)
    scores = jnp.einsum('nkgd,mkd->kgnm', grouped, keys.astype(jnp.float32)) * attn_scale
    capped = soft_cap * jnp.tanh(scores / soft_cap)
    spots = jnp.arange(count)
    allowed = spots[None, :] <= spots[:, None]
    weights = jnp.where(allowed, jnp.exp(capped), 0.0)
    probs = (weights / lax.optimization_barrier(jnp.sum(weights, axis=-1, keepdims=True))).astype(jnp.bfloat16)
    mixed = jnp.einsum('kgnm,mkd->nkgd', probs.astype(jnp.float32), values.astype(jnp.float32))
    return mixed.reshape(count, heads * head_dim).astype(jnp.bfloat16)

def reference(tokens, norm_gain, w_query, w_key, w_value, w_out, post_gain):
    local = tokens.astype(jnp.float32)
    total = lax.optimization_barrier(jnp.sum(local * local, axis=1))
    normed = (local * lax.rsqrt(total / D + eps_norm)[:, None] * norm_gain.astype(jnp.float32)).astype(jnp.bfloat16)
    query_raw = jnp.dot(normed, w_query, preferred_element_type=jnp.float32)
    key_raw = jnp.dot(normed, w_key, preferred_element_type=jnp.float32)
    value_raw = jnp.dot(normed, w_value, preferred_element_type=jnp.float32)
    position = (jnp.arange(TOKENS) % LEN).astype(jnp.int32)
    query = rotate(query_raw.reshape(TOKENS, HEADS, HEAD_DIM), position).astype(jnp.bfloat16)
    key = rotate(key_raw.reshape(TOKENS, KV_HEADS, HEAD_DIM), position).astype(jnp.bfloat16)
    value = value_raw.astype(jnp.bfloat16).reshape(TOKENS, KV_HEADS, HEAD_DIM)
    seq_count = TOKENS // LEN
    attn = lax.map(lambda item: attend(item[0], item[1], item[2]), (query.reshape(seq_count, LEN, HEADS, HEAD_DIM), key.reshape(seq_count, LEN, KV_HEADS, HEAD_DIM), value.reshape(seq_count, LEN, KV_HEADS, HEAD_DIM)))
    attn = attn.reshape(TOKENS, HEADS * HEAD_DIM)
    block = BLOCK_COLS
    proj = jnp.zeros((TOKENS, D), jnp.float32)
    for group in range(N_TENSOR):
        partial_value = jnp.dot(attn[:, group * block:(group + 1) * block], w_out[group * block:(group + 1) * block], preferred_element_type=jnp.float32)
        rounded = lax.optimization_barrier(partial_value.astype(jnp.bfloat16))
        proj = proj + rounded.astype(jnp.float32)
    post_total = lax.optimization_barrier(jnp.sum(proj * proj, axis=1))
    branch = proj * lax.rsqrt(post_total / D + eps_norm)[:, None] * post_gain.astype(jnp.float32)
    return local + branch
```

```python
import jax
import jax.numpy as jnp
from jax import lax
from jax.sharding import PartitionSpec as P

HEAD_DIM = 128

eps_norm = 1e-06
soft_cap = 50.0
attn_scale = 144.0 ** (-0.5)
rope_base = 10000.0


def rotate(values, position):
    head_dim = values.shape[-1]
    half = head_dim // 2
    freq = rope_base ** (-(jnp.arange(half, dtype=jnp.float32) * 2.0 / head_dim))
    angle = position.astype(jnp.float32)[:, None] * freq[None, :]
    cosine = jnp.cos(angle)[:, None, :]
    sine = jnp.sin(angle)[:, None, :]
    first = values[..., :half]
    second = values[..., half:]
    return jnp.concatenate(
        [first * cosine - second * sine, second * cosine + first * sine], axis=-1
    )


def attend(query, keys, values, position):
    count, heads, head_dim = query.shape
    kv_count = keys.shape[1]
    grouped = query.reshape(count, kv_count, heads // kv_count, head_dim)
    scores = (
        jnp.einsum("nkgd,mkd->kgnm", grouped, keys, preferred_element_type=jnp.float32) * attn_scale
    )
    capped = soft_cap * jnp.tanh(scores / soft_cap)
    allowed = position[None, :] <= position[:, None]
    weights = jnp.where(allowed, jnp.exp(capped), 0.0)
    probs = (weights / jnp.sum(weights, axis=-1, keepdims=True)).astype(jnp.bfloat16)
    mixed = jnp.einsum("kgnm,mkd->nkgd", probs, values, preferred_element_type=jnp.float32)
    return mixed.reshape(count, heads * head_dim).astype(jnp.bfloat16)


def swap_pairs(n_fsdp, n_tensor, turn):
    ratio = n_fsdp // n_tensor
    pairs = []
    for f in range(n_fsdp):
        for t in range(n_tensor):
            j = (f + turn) % ratio
            pairs.append((f * n_tensor + t, (t * ratio + j) * n_tensor + f // ratio))
    return pairs


def to_rows(block, n_fsdp, n_tensor):
    rows = block.shape[0]
    ratio = n_fsdp // n_tensor
    width = block.shape[1] // ratio
    f = lax.axis_index("fsdp")
    if ratio == 1:
        held = lax.ppermute(block, ("fsdp", "tensor"), swap_pairs(n_fsdp, n_tensor, 0))
    else:
        held = jnp.zeros((ratio, rows, width), block.dtype)
        for turn in range(ratio):
            piece = lax.dynamic_slice_in_dim(block, (f + turn) % ratio * width, width, 1)
            got = lax.ppermute(piece, ("fsdp", "tensor"), swap_pairs(n_fsdp, n_tensor, turn))
            held = lax.dynamic_update_index_in_dim(held, got, (f - turn) % ratio, 0)
        held = held.reshape(ratio * rows, width)
    return lax.all_gather(held, "tensor", axis=0, tiled=True)


def from_rows(summed, rows, n_fsdp, n_tensor):
    ratio = n_fsdp // n_tensor
    width = summed.shape[1]
    f = lax.axis_index("fsdp")
    back = lambda turn: [(b, a) for a, b in swap_pairs(n_fsdp, n_tensor, turn)]
    if ratio == 1:
        return lax.ppermute(summed, ("fsdp", "tensor"), back(0))
    pieces = summed.reshape(ratio, rows, width)
    out = jnp.zeros((rows, ratio * width), summed.dtype)
    for turn in range(ratio):
        piece = lax.dynamic_index_in_dim(pieces, (f - turn) % ratio, 0, keepdims=False)
        got = lax.ppermute(piece, ("fsdp", "tensor"), back(turn))
        out = lax.dynamic_update_slice_in_dim(out, got, (f + turn) % ratio * width, 1)
    return out


def solution(mesh):
    n_fsdp, n_tensor = mesh.shape["fsdp"], mesh.shape["tensor"]

    def on_device(tokens, norm_gain, w_query, w_key, w_value, w_out, post_gain):
        rows = tokens.shape[0]
        width = tokens.shape[1] * n_tensor
        widened = tokens.astype(jnp.float32)
        total = lax.psum(jnp.sum(widened * widened, axis=1), "tensor")
        normed = (
            widened * lax.rsqrt(total / width + eps_norm)[:, None] * norm_gain.astype(jnp.float32)
        ).astype(jnp.bfloat16)
        mine = to_rows(normed, n_fsdp, n_tensor)
        raw = []
        for piece in (w_query, w_key, w_value):
            part = jnp.dot(mine, piece, preferred_element_type=jnp.float32).astype(jnp.bfloat16)
            parts = lax.all_to_all(part, "fsdp", 0, 0, tiled=True)
            parts = parts.reshape(n_fsdp, rows, piece.shape[1])
            raw.append(jnp.sum(parts.astype(jnp.float32), axis=0))
        query_raw, key_raw, value_raw = raw
        position = jnp.arange(rows, dtype=jnp.int32)
        local_heads = w_query.shape[1] // HEAD_DIM
        local_kv = w_key.shape[1] // HEAD_DIM
        query = rotate(query_raw.reshape(rows, local_heads, HEAD_DIM), position)
        key = rotate(key_raw.reshape(rows, local_kv, HEAD_DIM), position)
        query, key = query.astype(jnp.bfloat16), key.astype(jnp.bfloat16)
        value = value_raw.astype(jnp.bfloat16).reshape(rows, local_kv, HEAD_DIM)
        attn = attend(query, key, value, position)
        attn_all = lax.all_gather(attn, "fsdp", axis=0, tiled=True)
        part = jnp.dot(attn_all, w_out, preferred_element_type=jnp.float32).astype(jnp.bfloat16)
        summed = lax.psum_scatter(part, "tensor", scatter_dimension=0, tiled=True)
        proj = from_rows(summed, rows, n_fsdp, n_tensor).astype(jnp.float32)
        post_total = lax.psum(jnp.sum(proj * proj, axis=1), "tensor")
        branch = (
            proj
            * lax.rsqrt(post_total / width + eps_norm)[:, None]
            * post_gain.astype(jnp.float32)
        )
        return tokens.astype(jnp.float32) + branch

    placed = (
        P(("groups", "fsdp"), "tensor"),
        P("tensor"),
        P("fsdp", "tensor"),
        P("fsdp", "tensor"),
        P("fsdp", "tensor"),
        P("tensor", "fsdp"),
        P("tensor"),
    )
    return jax.shard_map(
        on_device,
        mesh=mesh,
        in_specs=placed,
        out_specs=P(("groups", "fsdp"), "tensor"),
        check_vma=False,
    )
```

```python
import functools

import jax
import jax.numpy as jnp
from jax import lax
from jax.experimental import pallas as pl
from jax.experimental.pallas import tpu as pltpu
from jax.sharding import PartitionSpec as P

HEAD_DIM = 128

eps_norm = 1e-06
soft_cap = 50.0
attn_scale = 144.0 ** (-0.5)
rope_base = 10000.0


def rotate(values, position):
    head_dim = values.shape[-1]
    half = head_dim // 2
    freq = rope_base ** (-(jnp.arange(half, dtype=jnp.float32) * 2.0 / head_dim))
    angle = position.astype(jnp.float32)[:, None] * freq[None, :]
    cosine = jnp.cos(angle)[:, None, :]
    sine = jnp.sin(angle)[:, None, :]
    first = values[..., :half]
    second = values[..., half:]
    return jnp.concatenate(
        [first * cosine - second * sine, second * cosine + first * sine], axis=-1
    )


def attend(query, keys, values, position):
    count, heads, head_dim = query.shape
    kv_count = keys.shape[1]
    grouped = query.reshape(count, kv_count, heads // kv_count, head_dim)
    scores = (
        jnp.einsum("nkgd,mkd->kgnm", grouped, keys, preferred_element_type=jnp.float32) * attn_scale
    )
    capped = soft_cap * jnp.tanh(scores / soft_cap)
    allowed = position[None, :] <= position[:, None]
    weights = jnp.where(allowed, jnp.exp(capped), 0.0)
    probs = (weights / jnp.sum(weights, axis=-1, keepdims=True)).astype(jnp.bfloat16)
    mixed = jnp.einsum("kgnm,mkd->nkgd", probs, values, preferred_element_type=jnp.float32)
    return mixed.reshape(count, heads * head_dim).astype(jnp.bfloat16)


def swap_pairs(n_fsdp, n_tensor, turn):
    ratio = n_fsdp // n_tensor
    pairs = []
    for f in range(n_fsdp):
        for t in range(n_tensor):
            j = (f + turn) % ratio
            pairs.append((f * n_tensor + t, (t * ratio + j) * n_tensor + f // ratio))
    return pairs


def to_rows(block, n_fsdp, n_tensor):
    rows = block.shape[0]
    ratio = n_fsdp // n_tensor
    width = block.shape[1] // ratio
    f = lax.axis_index("fsdp")
    if ratio == 1:
        held = lax.ppermute(block, ("fsdp", "tensor"), swap_pairs(n_fsdp, n_tensor, 0))
    else:
        held = jnp.zeros((ratio, rows, width), block.dtype)
        for turn in range(ratio):
            piece = lax.dynamic_slice_in_dim(block, (f + turn) % ratio * width, width, 1)
            got = lax.ppermute(piece, ("fsdp", "tensor"), swap_pairs(n_fsdp, n_tensor, turn))
            held = lax.dynamic_update_index_in_dim(held, got, (f - turn) % ratio, 0)
        held = held.reshape(ratio * rows, width)
    return lax.all_gather(held, "tensor", axis=0, tiled=True)


def from_rows(summed, rows, n_fsdp, n_tensor):
    ratio = n_fsdp // n_tensor
    width = summed.shape[1]
    f = lax.axis_index("fsdp")
    back = lambda turn: [(b, a) for a, b in swap_pairs(n_fsdp, n_tensor, turn)]
    if ratio == 1:
        return lax.ppermute(summed, ("fsdp", "tensor"), back(0))
    pieces = summed.reshape(ratio, rows, width)
    out = jnp.zeros((rows, ratio * width), summed.dtype)
    for turn in range(ratio):
        piece = lax.dynamic_index_in_dim(pieces, (f - turn) % ratio, 0, keepdims=False)
        got = lax.ppermute(piece, ("fsdp", "tensor"), back(turn))
        out = lax.dynamic_update_slice_in_dim(out, got, (f + turn) % ratio * width, 1)
    return out


MESH = pl.DeviceIdType.MESH
VMEM_LIMIT = 60 * 1024 * 1024


def greet(n, f, t):
    barrier = pltpu.get_barrier_semaphore()

    def signal(a, b):
        pl.semaphore_signal(
            barrier, inc=1, device_id={"fsdp": a, "tensor": b}, device_id_type=MESH
        )

    for k in range(1, n):
        signal(f, lax.rem(t + k, n))
    pl.when(f != t)(lambda: signal(t, f))
    pl.when(f > 0)(lambda: signal(f - 1, t))
    pl.when(f < n - 1)(lambda: signal(f + 1, t))
    one, none = jnp.int32(1), jnp.int32(0)
    peers = n - 1
    for there in (f != t, f > 0, f < n - 1):
        peers = peers + jnp.where(there, one, none)
    pl.semaphore_wait(barrier, peers)


def remote(src, dst, send, recv, a, b):
    return pltpu.make_async_remote_copy(
        src_ref=src,
        dst_ref=dst,
        send_sem=send,
        recv_sem=recv,
        device_id={"fsdp": a, "tensor": b},
        device_id_type=MESH,
    )


def qkv_kernel(
    n, cuts, x_ref, wq_ref, wk_ref, wv_ref, out_ref,
    xs, from_low, from_high, stage,
    local_sem, turn_send, turn_recv, cast_send, cast_recv,
    up_send, up_recv, down_send, down_recv,
):
    f, t = lax.axis_index("fsdp"), lax.axis_index("tensor")
    rows = x_ref.shape[0]
    half = rows // cuts
    greet(n, f, t)

    def part_rows(h):
        return pl.ds(h * half, half)

    def turned(h, slot):
        return remote(
            x_ref.at[part_rows(h)], xs.at[slot, part_rows(h)],
            turn_send.at[h], turn_recv.at[h], t, f,
        )

    def kept():
        return pltpu.make_async_copy(x_ref, xs.at[t], local_sem)

    def cast(h, slot, k):
        return remote(
            xs.at[slot, part_rows(h)], xs.at[slot, part_rows(h)],
            cast_send.at[k - 1, h], cast_recv.at[slot, h], f, lax.rem(t + k, n),
        )

    @pl.when(f != t)
    def _():
        for h in range(cuts):
            turned(h, f).start()

    @pl.when(f == t)
    def _():
        kept().start()
        kept().wait()

    for h in range(cuts):
        pl.when(f != t)(lambda h=h: turned(h, f).wait_recv())
        for k in range(1, n):
            cast(h, t, k).start()

    def arrive(slot):
        @pl.when(slot != t)
        def _():
            for h in range(cuts):
                cast(h, slot, 1).wait_recv()

    wide = wk_ref.shape[1]
    count = wq_ref.shape[1] // wide + 2
    weights = [(wq_ref, i * wide) for i in range(count - 2)] + [(wk_ref, 0), (wv_ref, 0)]

    def partial(block, c):
        ref, start = weights[c]
        return jnp.dot(
            xs[block], ref[:, start : start + wide], preferred_element_type=jnp.float32
        )

    def up(d, c):
        return remote(
            stage.at[d, c], from_low.at[d, c], up_send.at[d, c], up_recv.at[d, c], lax.rem(f + 1, n), t
        )

    def down(d, c):
        return remote(
            stage.at[d, c], from_high.at[d, c], down_send.at[d, c], down_recv.at[d, c], lax.rem(f + n - 1, n), t
        )

    def widened(ref, d, c):
        return ref[d, c].astype(jnp.float32)

    def travel(d, c, copy, source, first):
        part = partial(d, c)

        @pl.when(first)
        def _():
            stage[d, c] = part.astype(stage.dtype)

        @pl.when(jnp.logical_not(first))
        def _():
            copy(d, c).wait_recv()
            stage[d, c] = (part + widened(source, d, c)).astype(stage.dtype)

        copy(d, c).start()

    def step(s, carry):
        high, low = n - 1 - s, s
        pl.when(high > f)(lambda: arrive(high))
        pl.when((low < f))(lambda: arrive(low))
        for c in range(count):
            pl.when(high > f)(lambda c=c: travel(high, c, up, from_low, f == 0))
            pl.when(low < f)(lambda c=c: travel(low, c, down, from_high, f == n - 1))
        return carry

    lax.fori_loop(0, n - 1, step, 0)
    arrive(f)
    for c in range(count):
        cols = slice(c * wide, (c + 1) * wide)
        out_ref[:, cols] = partial(f, c)

        @pl.when(f > 0)
        def _():
            up(f, c).wait_recv()
            out_ref[:, cols] += widened(from_low, f, c)

        @pl.when(f < n - 1)
        def _():
            down(f, c).wait_recv()
            out_ref[:, cols] += widened(from_high, f, c)

    def drain(d, carry):
        for c in range(count):
            pl.when(d > f)(lambda c=c: up(d, c).wait_send())
            pl.when(d < f)(lambda c=c: down(d, c).wait_send())
        return carry

    lax.fori_loop(0, n, drain, 0)
    for h in range(cuts):
        pl.when(f != t)(lambda h=h: turned(h, f).wait_send())
        for k in range(1, n):
            cast(h, t, k).wait_send()


def out_kernel(
    n, cuts, kv, raw_ref, cos_ref, sin_ref, w_ref, out_ref,
    att, stage, got, merged, landed,
    up_send, up_recv, down_send, down_recv, plane_send, plane_recv, turn_send, turn_recv,
):
    f, t = lax.axis_index("fsdp"), lax.axis_index("tensor")
    rows = raw_ref.shape[0]
    half = rows // cuts
    greet(n, f, t)
    heads = w_ref.shape[0] // HEAD_DIM
    per = heads // kv
    wide = per * HEAD_DIM

    def up(src, h):
        return remote(
            att.at[src, h], att.at[src, h], up_send.at[src, h], up_recv.at[src, h], lax.rem(f + 1, n), t
        )

    def down(src, h):
        return remote(
            att.at[src, h], att.at[src, h], down_send.at[src, h], down_recv.at[src, h], lax.rem(f + n - 1, n), t
        )

    def turn(u):
        return (u * cos_ref[...] + pltpu.roll(u, HEAD_DIM // 2, 1) * sin_ref[...]).astype(
            jnp.bfloat16
        )

    def piece(start):
        return raw_ref[:, start : start + HEAD_DIM]

    query_at = lax.broadcasted_iota(jnp.int32, (rows, rows), 0)
    key_at = lax.broadcasted_iota(jnp.int32, (rows, rows), 1)
    allowed = key_at <= query_at
    for h in range(kv):
        key = turn(piece((heads + h) * HEAD_DIM))
        value = piece((heads + kv + h) * HEAD_DIM).astype(jnp.bfloat16)
        for g in range(per):
            query = turn(piece((h * per + g) * HEAD_DIM))
            scores = lax.dot_general(
                query, key, (((1,), (1,)), ((), ())), preferred_element_type=jnp.float32
            ) * attn_scale
            capped = soft_cap * jnp.tanh(scores / soft_cap)
            e = jnp.where(allowed, jnp.exp(capped), 0.0)
            probs = (e / jnp.sum(e, axis=1, keepdims=True)).astype(jnp.bfloat16)
            mixed = jnp.dot(probs, value, preferred_element_type=jnp.float32)
            att[f, h, :, g * HEAD_DIM : (g + 1) * HEAD_DIM] = mixed.astype(jnp.bfloat16)
        pl.when(f < n - 1)(lambda h=h: up(f, h).start())
        pl.when(f > 0)(lambda h=h: down(f, h).start())

    def part_rows(r):
        return pl.ds(r * half, half)

    def plane(d, r, slot):
        return remote(
            stage.at[d, part_rows(r)], got.at[slot, part_rows(r)],
            plane_send.at[d, r], plane_recv.at[slot, r], f, d,
        )

    def project(d):
        for r in range(cuts):
            span = slice(r * half, (r + 1) * half)
            total = jnp.dot(
                att[d, 0, span], w_ref[0:wide], preferred_element_type=jnp.float32
            )
            for h in range(1, kv):
                total += jnp.dot(
                    att[d, h, span],
                    w_ref[h * wide : (h + 1) * wide],
                    preferred_element_type=jnp.float32,
                )
            stage[d, span] = total.astype(stage.dtype)
            pl.when(d != t)(lambda r=r: plane(d, r, t).start())

    project(f)

    def step(s, carry):
        low, high = f - s, f + s

        for h in range(kv):

            @pl.when(low >= 0)
            def _():
                up(low, h).wait_recv()
                pl.when(f < n - 1)(lambda: up(low, h).start())

            @pl.when(high < n)
            def _():
                down(high, h).wait_recv()
                pl.when(f > 0)(lambda: down(high, h).start())

        pl.when(low >= 0)(lambda: project(low))
        pl.when(high < n)(lambda: project(high))
        return carry

    lax.fori_loop(1, n, step, 0)

    def back(r):
        return remote(
            merged.at[part_rows(r)], landed.at[part_rows(r)],
            turn_send.at[r], turn_recv.at[r], t, f,
        )

    for r in range(cuts):
        span = slice(r * half, (r + 1) * half)
        total = stage[t, span].astype(jnp.float32)
        for k in range(1, n):
            slot = lax.rem(t + k, n)
            plane(slot, r, slot).wait_recv()
            total += got[slot, span].astype(jnp.float32)
        merged[span] = total.astype(merged.dtype)
        pl.when(f != t)(lambda r=r: back(r).start())
    for r in range(cuts):
        span = slice(r * half, (r + 1) * half)

        @pl.when(f == t)
        def _():
            out_ref[span] = merged[span]

        @pl.when(f != t)
        def _():
            back(r).wait_recv()
            out_ref[span] = landed[span]
            back(r).wait_send()

    def drain(d, carry):
        for h in range(kv):
            pl.when((d <= f) & (f < n - 1))(lambda h=h: up(d, h).wait_send())
            pl.when((d >= f) & (f > 0))(lambda h=h: down(d, h).wait_send())
        for r in range(cuts):
            pl.when(d != t)(lambda r=r: plane(d, r, t).wait_send())
        return carry

    lax.fori_loop(0, n, drain, 0)


def in_vmem(count):
    return [pl.BlockSpec(memory_space=pltpu.VMEM)] * count


def project_in(n, normed, w_query, w_key, w_value):
    rows, width = normed.shape
    wide = w_key.shape[1]
    count = w_query.shape[1] // wide + 2
    cuts = 4
    block = (n, count, rows, wide)
    dma = pltpu.SemaphoreType.DMA
    return pl.pallas_call(
        functools.partial(qkv_kernel, n, cuts),
        out_shape=jax.ShapeDtypeStruct((rows, count * wide), jnp.float32),
        in_specs=in_vmem(4),
        out_specs=pl.BlockSpec(memory_space=pltpu.VMEM),
        scratch_shapes=[
            pltpu.VMEM((n, rows, width), jnp.bfloat16),
            pltpu.VMEM(block, jnp.bfloat16),
            pltpu.VMEM(block, jnp.bfloat16),
            pltpu.VMEM(block, jnp.bfloat16),
            dma(()), dma((cuts,)), dma((cuts,)), dma((n - 1, cuts)), dma((n, cuts)),
            dma((n, count)), dma((n, count)), dma((n, count)), dma((n, count)),
        ],
        compiler_params=pltpu.CompilerParams(
            collective_id=0, has_side_effects=True, vmem_limit_bytes=VMEM_LIMIT
        ),
    )(normed, w_query, w_key, w_value)


def project_out(n, raw, cosine, sine, w_out, kv):
    rows = raw.shape[0]
    width = w_out.shape[1]
    cuts = 2
    wide = w_out.shape[0] // kv
    dma = pltpu.SemaphoreType.DMA
    return pl.pallas_call(
        functools.partial(out_kernel, n, cuts, kv),
        out_shape=jax.ShapeDtypeStruct((rows, width), jnp.bfloat16),
        in_specs=in_vmem(4),
        out_specs=pl.BlockSpec(memory_space=pltpu.VMEM),
        scratch_shapes=[
            pltpu.VMEM((n, kv, rows, wide), jnp.bfloat16),
            pltpu.VMEM((n, rows, width), jnp.bfloat16),
            pltpu.VMEM((n, rows, width), jnp.bfloat16),
            pltpu.VMEM((rows, width), jnp.bfloat16),
            pltpu.VMEM((rows, width), jnp.bfloat16),
            dma((n, kv)), dma((n, kv)), dma((n, kv)), dma((n, kv)),
            dma((n, cuts)), dma((n, cuts)), dma((cuts,)), dma((cuts,)),
        ],
        compiler_params=pltpu.CompilerParams(
            collective_id=1, has_side_effects=True, vmem_limit_bytes=VMEM_LIMIT
        ),
    )(raw, cosine, sine, w_out)


def tables(rows):
    half = HEAD_DIM // 2
    freq = rope_base ** (-(jnp.arange(half, dtype=jnp.float32) * 2.0 / HEAD_DIM))
    angle = jnp.arange(rows, dtype=jnp.int32).astype(jnp.float32)[:, None] * freq[None, :]
    cosine, sine = jnp.cos(angle), jnp.sin(angle)
    return jnp.concatenate([cosine, cosine], axis=1), jnp.concatenate([-sine, sine], axis=1)


def solution(mesh):
    n_fsdp, n_tensor = mesh.shape["fsdp"], mesh.shape["tensor"]

    def on_device(tokens, norm_gain, w_query, w_key, w_value, w_out, post_gain):
        rows = tokens.shape[0]
        width = tokens.shape[1] * n_tensor
        widened = tokens.astype(jnp.float32)
        total = lax.psum(jnp.sum(widened * widened, axis=1), "tensor")
        normed = (
            widened * lax.rsqrt(total / width + eps_norm)[:, None] * norm_gain.astype(jnp.float32)
        ).astype(jnp.bfloat16)
        if n_fsdp == n_tensor:
            kv = w_key.shape[1] // HEAD_DIM
            raw = project_in(n_fsdp, normed, w_query, w_key, w_value)
            proj = project_out(n_fsdp, raw, *tables(rows), w_out, kv).astype(jnp.float32)
        else:
            mine = to_rows(normed, n_fsdp, n_tensor)
            raw = []
            for piece in (w_query, w_key, w_value):
                part = jnp.dot(mine, piece, preferred_element_type=jnp.float32).astype(jnp.bfloat16)
                parts = lax.all_to_all(part, "fsdp", 0, 0, tiled=True)
                parts = parts.reshape(n_fsdp, rows, piece.shape[1])
                raw.append(jnp.sum(parts.astype(jnp.float32), axis=0))
            query_raw, key_raw, value_raw = raw
            position = jnp.arange(rows, dtype=jnp.int32)
            local_heads = w_query.shape[1] // HEAD_DIM
            local_kv = w_key.shape[1] // HEAD_DIM
            query = rotate(query_raw.reshape(rows, local_heads, HEAD_DIM), position)
            key = rotate(key_raw.reshape(rows, local_kv, HEAD_DIM), position)
            query, key = query.astype(jnp.bfloat16), key.astype(jnp.bfloat16)
            value = value_raw.astype(jnp.bfloat16).reshape(rows, local_kv, HEAD_DIM)
            attn = attend(query, key, value, position)
            attn_all = lax.all_gather(attn, "fsdp", axis=0, tiled=True)
            part = jnp.dot(attn_all, w_out, preferred_element_type=jnp.float32).astype(jnp.bfloat16)
            summed = lax.psum_scatter(part, "tensor", scatter_dimension=0, tiled=True)
            proj = from_rows(summed, rows, n_fsdp, n_tensor).astype(jnp.float32)
        post_total = lax.psum(jnp.sum(proj * proj, axis=1), "tensor")
        branch = (
            proj
            * lax.rsqrt(post_total / width + eps_norm)[:, None]
            * post_gain.astype(jnp.float32)
        )
        return tokens.astype(jnp.float32) + branch

    placed = (
        P(("groups", "fsdp"), "tensor"),
        P("tensor"),
        P("fsdp", "tensor"),
        P("fsdp", "tensor"),
        P("fsdp", "tensor"),
        P("tensor", "fsdp"),
        P("tensor"),
    )
    return jax.shard_map(
        on_device,
        mesh=mesh,
        in_specs=placed,
        out_specs=P(("groups", "fsdp"), "tensor"),
        check_vma=False,
    )
```

```python
import functools

import jax
import jax.numpy as jnp
from jax import lax
from jax.experimental import pallas as pl
from jax.experimental.pallas import tpu as pltpu
from jax.sharding import PartitionSpec as P

HEAD_DIM = 128

eps_norm = 1e-06
soft_cap = 50.0
attn_scale = 144.0 ** (-0.5)
rope_base = 10000.0


def rotate(values, position):
    head_dim = values.shape[-1]
    half = head_dim // 2
    freq = rope_base ** (-(jnp.arange(half, dtype=jnp.float32) * 2.0 / head_dim))
    angle = position.astype(jnp.float32)[:, None] * freq[None, :]
    cosine = jnp.cos(angle)[:, None, :]
    sine = jnp.sin(angle)[:, None, :]
    first = values[..., :half]
    second = values[..., half:]
    return jnp.concatenate(
        [first * cosine - second * sine, second * cosine + first * sine], axis=-1
    )


def attend(query, keys, values, position):
    count, heads, head_dim = query.shape
    kv_count = keys.shape[1]
    grouped = query.reshape(count, kv_count, heads // kv_count, head_dim)
    scores = (
        jnp.einsum("nkgd,mkd->kgnm", grouped, keys, preferred_element_type=jnp.float32) * attn_scale
    )
    capped = soft_cap * jnp.tanh(scores / soft_cap)
    allowed = position[None, :] <= position[:, None]
    weights = jnp.where(allowed, jnp.exp(capped), 0.0)
    probs = (weights / jnp.sum(weights, axis=-1, keepdims=True)).astype(jnp.bfloat16)
    mixed = jnp.einsum("kgnm,mkd->nkgd", probs, values, preferred_element_type=jnp.float32)
    return mixed.reshape(count, heads * head_dim).astype(jnp.bfloat16)


def swap_pairs(n_fsdp, n_tensor, turn):
    ratio = n_fsdp // n_tensor
    pairs = []
    for f in range(n_fsdp):
        for t in range(n_tensor):
            j = (f + turn) % ratio
            pairs.append((f * n_tensor + t, (t * ratio + j) * n_tensor + f // ratio))
    return pairs


def to_rows(block, n_fsdp, n_tensor):
    rows = block.shape[0]
    ratio = n_fsdp // n_tensor
    width = block.shape[1] // ratio
    f = lax.axis_index("fsdp")
    if ratio == 1:
        held = lax.ppermute(block, ("fsdp", "tensor"), swap_pairs(n_fsdp, n_tensor, 0))
    else:
        held = jnp.zeros((ratio, rows, width), block.dtype)
        for turn in range(ratio):
            piece = lax.dynamic_slice_in_dim(block, (f + turn) % ratio * width, width, 1)
            got = lax.ppermute(piece, ("fsdp", "tensor"), swap_pairs(n_fsdp, n_tensor, turn))
            held = lax.dynamic_update_index_in_dim(held, got, (f - turn) % ratio, 0)
        held = held.reshape(ratio * rows, width)
    return lax.all_gather(held, "tensor", axis=0, tiled=True)


def from_rows(summed, rows, n_fsdp, n_tensor):
    ratio = n_fsdp // n_tensor
    width = summed.shape[1]
    f = lax.axis_index("fsdp")
    back = lambda turn: [(b, a) for a, b in swap_pairs(n_fsdp, n_tensor, turn)]
    if ratio == 1:
        return lax.ppermute(summed, ("fsdp", "tensor"), back(0))
    pieces = summed.reshape(ratio, rows, width)
    out = jnp.zeros((rows, ratio * width), summed.dtype)
    for turn in range(ratio):
        piece = lax.dynamic_index_in_dim(pieces, (f - turn) % ratio, 0, keepdims=False)
        got = lax.ppermute(piece, ("fsdp", "tensor"), back(turn))
        out = lax.dynamic_update_slice_in_dim(out, got, (f + turn) % ratio * width, 1)
    return out


MESH = pl.DeviceIdType.MESH
VMEM_LIMIT = 60 * 1024 * 1024


def greet(n, f, t):
    barrier = pltpu.get_barrier_semaphore()

    def signal(a, b):
        pl.semaphore_signal(
            barrier, inc=1, device_id={"fsdp": a, "tensor": b}, device_id_type=MESH
        )

    for k in range(1, n):
        signal(f, lax.rem(t + k, n))
    pl.when(f != t)(lambda: signal(t, f))
    pl.when(f > 0)(lambda: signal(f - 1, t))
    pl.when(f < n - 1)(lambda: signal(f + 1, t))
    one, none = jnp.int32(1), jnp.int32(0)
    peers = n - 1
    for there in (f != t, f > 0, f < n - 1):
        peers = peers + jnp.where(there, one, none)
    pl.semaphore_wait(barrier, peers)


def remote(src, dst, send, recv, a, b):
    return pltpu.make_async_remote_copy(
        src_ref=src,
        dst_ref=dst,
        send_sem=send,
        recv_sem=recv,
        device_id={"fsdp": a, "tensor": b},
        device_id_type=MESH,
    )


def qkv_kernel(
    n, cuts, sweeps, x_ref, wq_ref, wk_ref, wv_ref, out_ref,
    xs, from_low, from_high, stage,
    local_sem, turn_send, turn_recv, cast_send, cast_recv,
    up_send, up_recv, down_send, down_recv,
):
    f, t = lax.axis_index("fsdp"), lax.axis_index("tensor")
    rows = x_ref.shape[0]
    half = rows // cuts
    greet(n, f, t)

    def part_rows(h):
        start = h * half
        return pl.ds(start if isinstance(h, int) else pl.multiple_of(start, half), half)

    def turned(h, slot):
        return remote(
            x_ref.at[part_rows(h)], xs.at[slot, part_rows(h)],
            turn_send.at[h], turn_recv.at[h], t, f,
        )

    def kept():
        return pltpu.make_async_copy(x_ref, xs.at[t], local_sem)

    def cast(h, slot, k):
        return remote(
            xs.at[slot, part_rows(h)], xs.at[slot, part_rows(h)],
            cast_send.at[k - 1, h], cast_recv.at[slot, h], f, lax.rem(t + k, n),
        )

    @pl.when(f != t)
    def _():
        for h in range(cuts):
            turned(h, f).start()

    @pl.when(f == t)
    def _():
        kept().start()
        kept().wait()

    def spread(r):
        for i in range(cuts // sweeps):
            h = r * (cuts // sweeps) + i
            pl.when(f != t)(lambda h=h: turned(h, f).wait_recv())
            for k in range(1, n):
                cast(h, t, k).start()

    spread(0)

    span = rows // sweeps
    each = cuts // sweeps

    def arrive(slot, r):
        @pl.when(slot != t)
        def _():
            for h in range(each):
                cast(r * each + h, slot, 1).wait_recv()

    def swept(r):
        return pl.ds(pl.multiple_of(r * span, span), span)

    wide = wk_ref.shape[1]
    count = wq_ref.shape[1] // wide + 2
    weights = [(wq_ref, i * wide) for i in range(count - 2)] + [(wk_ref, 0), (wv_ref, 0)]

    def partial(block, c, r):
        ref, start = weights[c]
        return jnp.dot(
            xs[block, swept(r)],
            ref[:, start : start + wide],
            preferred_element_type=jnp.float32,
        )

    def up(d, c, r):
        return remote(
            stage.at[d, c, swept(r)], from_low.at[d, c, swept(r)],
            up_send.at[d, c, r], up_recv.at[d, c, r], lax.rem(f + 1, n), t,
        )

    def down(d, c, r):
        return remote(
            stage.at[d, c, swept(r)], from_high.at[d, c, swept(r)],
            down_send.at[d, c, r], down_recv.at[d, c, r], lax.rem(f + n - 1, n), t,
        )

    def widened(ref, d, c, r):
        return ref[d, c, swept(r)].astype(jnp.float32)

    def travel(d, c, r, copy, source, first):
        part = partial(d, c, r)

        @pl.when(first)
        def _():
            stage[d, c, swept(r)] = part.astype(stage.dtype)

        @pl.when(jnp.logical_not(first))
        def _():
            copy(d, c, r).wait_recv()
            stage[d, c, swept(r)] = (part + widened(source, d, c, r)).astype(stage.dtype)

        copy(d, c, r).start()

    def sweep(r, outer):
        def step(s, carry):
            high, low = n - 1 - s, s
            pl.when(high > f)(lambda: arrive(high, r))
            pl.when(low < f)(lambda: arrive(low, r))
            for c in range(count):
                pl.when(high > f)(lambda c=c: travel(high, c, r, up, from_low, f == 0))
                pl.when(low < f)(lambda c=c: travel(low, c, r, down, from_high, f == n - 1))
            pl.when((s == 0) & (r + 1 < sweeps))(lambda: spread(r + 1))
            return carry

        return lax.fori_loop(0, n - 1, step, outer)

    def finish(r, carry):
        arrive(f, r)
        for c in range(count):
            cols = slice(c * wide, (c + 1) * wide)
            out_ref[swept(r), cols] = partial(f, c, r)

            @pl.when(f > 0)
            def _():
                up(f, c, r).wait_recv()
                out_ref[swept(r), cols] += widened(from_low, f, c, r)

            @pl.when(f < n - 1)
            def _():
                down(f, c, r).wait_recv()
                out_ref[swept(r), cols] += widened(from_high, f, c, r)

        return carry

    lax.fori_loop(0, sweeps, sweep, 0)
    lax.fori_loop(0, sweeps, finish, 0)

    def drain(d, carry):
        for c in range(count):
            for r in range(sweeps):
                pl.when(d > f)(lambda c=c, r=r: up(d, c, r).wait_send())
                pl.when(d < f)(lambda c=c, r=r: down(d, c, r).wait_send())
        return carry

    lax.fori_loop(0, n, drain, 0)
    for h in range(cuts):
        pl.when(f != t)(lambda h=h: turned(h, f).wait_send())
        for k in range(1, n):
            cast(h, t, k).wait_send()


def out_kernel(
    n, cuts, kv, raw_ref, cos_ref, sin_ref, w_ref, out_ref,
    att, stage, got, merged, landed,
    up_send, up_recv, down_send, down_recv, plane_send, plane_recv, turn_send, turn_recv,
):
    f, t = lax.axis_index("fsdp"), lax.axis_index("tensor")
    rows = raw_ref.shape[0]
    half = rows // cuts
    greet(n, f, t)
    heads = w_ref.shape[0] // HEAD_DIM
    per = heads // kv

    def part_rows(r):
        return pl.ds(r * half, half)

    def up(src, r):
        return remote(
            att.at[src, part_rows(r)], att.at[src, part_rows(r)],
            up_send.at[src, r], up_recv.at[src, r], lax.rem(f + 1, n), t,
        )

    def down(src, r):
        return remote(
            att.at[src, part_rows(r)], att.at[src, part_rows(r)],
            down_send.at[src, r], down_recv.at[src, r], lax.rem(f + n - 1, n), t,
        )

    def turn_rows(u, span):
        other = pltpu.roll(u, HEAD_DIM // 2, 1)
        return (u * cos_ref[span] + other * sin_ref[span]).astype(jnp.bfloat16)

    def turn(u):
        return turn_rows(u, slice(0, rows))

    def piece(start):
        return raw_ref[:, start : start + HEAD_DIM]

    keys = [turn(piece((heads + h) * HEAD_DIM)) for h in range(kv)]
    values = [piece((heads + kv + h) * HEAD_DIM).astype(jnp.bfloat16) for h in range(kv)]
    for r in range(cuts):
        span, seen = slice(r * half, (r + 1) * half), (r + 1) * half
        query_at = r * half + lax.broadcasted_iota(jnp.int32, (half, seen), 0)
        allowed = lax.broadcasted_iota(jnp.int32, (half, seen), 1) <= query_at
        for g in range(heads):
            h = g // per
            query = turn_rows(piece(g * HEAD_DIM)[span], span)
            scores = lax.dot_general(
                query, keys[h][:seen], (((1,), (1,)), ((), ())),
                preferred_element_type=jnp.float32,
            ) * attn_scale
            capped = soft_cap * jnp.tanh(scores / soft_cap)
            e = jnp.where(allowed, jnp.exp(capped), 0.0)
            probs = (e / jnp.sum(e, axis=1, keepdims=True)).astype(jnp.bfloat16)
            mixed = jnp.dot(probs, values[h][:seen], preferred_element_type=jnp.float32)
            att[f, span, g * HEAD_DIM : (g + 1) * HEAD_DIM] = mixed.astype(jnp.bfloat16)
        pl.when(f < n - 1)(lambda r=r: up(f, r).start())
        pl.when(f > 0)(lambda r=r: down(f, r).start())

    def plane(d, r, slot):
        return remote(
            stage.at[d, part_rows(r)], got.at[slot, part_rows(r)],
            plane_send.at[d, r], plane_recv.at[slot, r], f, d,
        )

    def project(d, r):
        span = slice(r * half, (r + 1) * half)
        total = jnp.dot(att[d, span], w_ref[...], preferred_element_type=jnp.float32)
        stage[d, span] = total.astype(stage.dtype)
        pl.when(d != t)(lambda: plane(d, r, t).start())

    def step(s, r):
        low, high = f - s, f + s

        @pl.when(low >= 0)
        def _():
            up(low, r).wait_recv()
            pl.when(f < n - 1)(lambda: up(low, r).start())

        @pl.when(high < n)
        def _():
            down(high, r).wait_recv()
            pl.when(f > 0)(lambda: down(high, r).start())

        pl.when(low >= 0)(lambda: project(low, r))
        pl.when(high < n)(lambda: project(high, r))

    def back(r):
        return remote(
            merged.at[part_rows(r)], landed.at[part_rows(r)],
            turn_send.at[r], turn_recv.at[r], t, f,
        )

    def merge(r):
        span = slice(r * half, (r + 1) * half)
        total = stage[t, span].astype(jnp.float32)
        for k in range(1, n):
            slot = lax.rem(t + k, n)
            plane(slot, r, slot).wait_recv()
            total += got[slot, span].astype(jnp.float32)
        merged[span] = total.astype(merged.dtype)
        pl.when(f != t)(lambda: back(r).start())

    for r in range(cuts):
        project(f, r)
        for s in range(1, n):
            step(s, r)
            if s == 1 and r > 0:
                merge(r - 1)
    merge(cuts - 1)
    for r in range(cuts):
        span = slice(r * half, (r + 1) * half)

        @pl.when(f == t)
        def _():
            out_ref[span] = merged[span]

        @pl.when(f != t)
        def _():
            back(r).wait_recv()
            out_ref[span] = landed[span]
            back(r).wait_send()

    def drain(d, carry):
        for r in range(cuts):
            pl.when((d <= f) & (f < n - 1))(lambda r=r: up(d, r).wait_send())
            pl.when((d >= f) & (f > 0))(lambda r=r: down(d, r).wait_send())
            pl.when(d != t)(lambda r=r: plane(d, r, t).wait_send())
        return carry

    lax.fori_loop(0, n, drain, 0)


def in_vmem(count):
    return [pl.BlockSpec(memory_space=pltpu.VMEM)] * count


def project_in(n, normed, w_query, w_key, w_value):
    rows, width = normed.shape
    wide = w_key.shape[1]
    count = w_query.shape[1] // wide + 2
    cuts, sweeps = 4, 2
    block = (n, count, rows, wide)
    dma = pltpu.SemaphoreType.DMA
    return pl.pallas_call(
        functools.partial(qkv_kernel, n, cuts, sweeps),
        out_shape=jax.ShapeDtypeStruct((rows, count * wide), jnp.float32),
        in_specs=in_vmem(4),
        out_specs=pl.BlockSpec(memory_space=pltpu.VMEM),
        scratch_shapes=[
            pltpu.VMEM((n, rows, width), jnp.bfloat16),
            pltpu.VMEM(block, jnp.bfloat16),
            pltpu.VMEM(block, jnp.bfloat16),
            pltpu.VMEM(block, jnp.bfloat16),
            dma(()), dma((cuts,)), dma((cuts,)), dma((n - 1, cuts)), dma((n, cuts)),
            *[dma((n, count, sweeps))] * 4,
        ],
        compiler_params=pltpu.CompilerParams(
            collective_id=0, has_side_effects=True, vmem_limit_bytes=VMEM_LIMIT
        ),
    )(normed, w_query, w_key, w_value)


def project_out(n, raw, cosine, sine, w_out, kv):
    rows = raw.shape[0]
    width = w_out.shape[1]
    cuts = 2
    dma = pltpu.SemaphoreType.DMA
    return pl.pallas_call(
        functools.partial(out_kernel, n, cuts, kv),
        out_shape=jax.ShapeDtypeStruct((rows, width), jnp.bfloat16),
        in_specs=in_vmem(4),
        out_specs=pl.BlockSpec(memory_space=pltpu.VMEM),
        scratch_shapes=[
            pltpu.VMEM((n, rows, w_out.shape[0]), jnp.bfloat16),
            pltpu.VMEM((n, rows, width), jnp.bfloat16),
            pltpu.VMEM((n, rows, width), jnp.bfloat16),
            pltpu.VMEM((rows, width), jnp.bfloat16),
            pltpu.VMEM((rows, width), jnp.bfloat16),
            *[dma((n, cuts))] * 4,
            dma((n, cuts)), dma((n, cuts)), dma((cuts,)), dma((cuts,)),
        ],
        compiler_params=pltpu.CompilerParams(
            collective_id=1, has_side_effects=True, vmem_limit_bytes=VMEM_LIMIT
        ),
    )(raw, cosine, sine, w_out)


def tables(rows):
    half = HEAD_DIM // 2
    freq = rope_base ** (-(jnp.arange(half, dtype=jnp.float32) * 2.0 / HEAD_DIM))
    angle = jnp.arange(rows, dtype=jnp.int32).astype(jnp.float32)[:, None] * freq[None, :]
    cosine, sine = jnp.cos(angle), jnp.sin(angle)
    return jnp.concatenate([cosine, cosine], axis=1), jnp.concatenate([-sine, sine], axis=1)


def solution(mesh):
    n_fsdp, n_tensor = mesh.shape["fsdp"], mesh.shape["tensor"]

    def on_device(tokens, norm_gain, w_query, w_key, w_value, w_out, post_gain):
        rows = tokens.shape[0]
        width = tokens.shape[1] * n_tensor
        widened = tokens.astype(jnp.float32)
        total = lax.psum(jnp.sum(widened * widened, axis=1), "tensor")
        normed = (
            widened * lax.rsqrt(total / width + eps_norm)[:, None] * norm_gain.astype(jnp.float32)
        ).astype(jnp.bfloat16)
        if n_fsdp == n_tensor:
            kv = w_key.shape[1] // HEAD_DIM
            raw = project_in(n_fsdp, normed, w_query, w_key, w_value)
            proj = project_out(n_fsdp, raw, *tables(rows), w_out, kv).astype(jnp.float32)
        else:
            mine = to_rows(normed, n_fsdp, n_tensor)
            raw = []
            for piece in (w_query, w_key, w_value):
                part = jnp.dot(mine, piece, preferred_element_type=jnp.float32).astype(jnp.bfloat16)
                parts = lax.all_to_all(part, "fsdp", 0, 0, tiled=True)
                parts = parts.reshape(n_fsdp, rows, piece.shape[1])
                raw.append(jnp.sum(parts.astype(jnp.float32), axis=0))
            query_raw, key_raw, value_raw = raw
            position = jnp.arange(rows, dtype=jnp.int32)
            local_heads = w_query.shape[1] // HEAD_DIM
            local_kv = w_key.shape[1] // HEAD_DIM
            query = rotate(query_raw.reshape(rows, local_heads, HEAD_DIM), position)
            key = rotate(key_raw.reshape(rows, local_kv, HEAD_DIM), position)
            query, key = query.astype(jnp.bfloat16), key.astype(jnp.bfloat16)
            value = value_raw.astype(jnp.bfloat16).reshape(rows, local_kv, HEAD_DIM)
            attn = attend(query, key, value, position)
            attn_all = lax.all_gather(attn, "fsdp", axis=0, tiled=True)
            part = jnp.dot(attn_all, w_out, preferred_element_type=jnp.float32).astype(jnp.bfloat16)
            summed = lax.psum_scatter(part, "tensor", scatter_dimension=0, tiled=True)
            proj = from_rows(summed, rows, n_fsdp, n_tensor).astype(jnp.float32)
        post_total = lax.psum(jnp.sum(proj * proj, axis=1), "tensor")
        branch = (
            proj
            * lax.rsqrt(post_total / width + eps_norm)[:, None]
            * post_gain.astype(jnp.float32)
        )
        return tokens.astype(jnp.float32) + branch

    placed = (
        P(("groups", "fsdp"), "tensor"),
        P("tensor"),
        P("fsdp", "tensor"),
        P("fsdp", "tensor"),
        P("fsdp", "tensor"),
        P("tensor", "fsdp"),
        P("tensor"),
    )
    return jax.shard_map(
        on_device,
        mesh=mesh,
        in_specs=placed,
        out_specs=P(("groups", "fsdp"), "tensor"),
        check_vma=False,
    )
```
